256 devices in a mesh: groups: 4 (over x, y), blk: 64 (over z, core).
Axes of the slice: x: 2, y: 2, z: 32, core: 2. Of those that a mesh axis runs over, the one named last changes fastest.
The devices are a block of a 4x8x32 slice.
Arguments:
- queries: bfloat16 [32768, 4096], P(('groups', 'blk')), parts along dimension 0, may hold values from -96 to 96
- keys: bfloat16 [32768, 512], P(('groups', 'blk')), parts along dimension 0, may hold values from -3 to 3
- values: bfloat16 [32768, 512], P(('groups', 'blk')), parts along dimension 0, may hold values from -4 to 4
- out_packed: int32 [4096, 512], P('blk'), may hold values from -2147483648 to 2147483646
- out_scales: bfloat16 [32, 4096], replicated, may hold values from 0.0029907227 to 0.029907227
- hadamard_signs: int32 [4096], replicated, may hold values from 0 to 1
Outputs:
- mixed: bfloat16 [32768, 4096], P(('groups', 'blk')), parts along dimension 0
The draws below stay inside these ranges and needn't reach their ends.
There are 4 independent parts, one for each index of `groups`. The reference program is written for one: setup_inputs(seed, part) draws one part's arguments, and reference() takes and returns one part's arrays. A program takes and returns all parts, laid end to end along the dimension named above; an argument that names none is the same for every part. Nothing has to cross between parts.
All inputs are finite; a program needn't handle non-finite values.
Results may differ from the reference program's by a relative error of at most 0.012.
Values may be sent and summed in bfloat16 or wider, within the bound.
No kernel may reach another device: no remote copies, remote signals or barrier semaphores. Data moves between devices by JAX's collectives and lax.ppermute only.
A program may use at most 256 MiB of HBM per device.

```python
import math
import jax
import jax.numpy as jnp
from jax import lax

HEAD_SIZE = 128
QUERY_HEADS = 32
KEY_VALUE_HEADS = 4
DO = 4096
GROUP = 128
SEQUENCE_LENGTH = 8192


def make_pair(key):
    base = jax.random.fold_in(key, 31)
    key_query, key_keys = jax.random.split(base, 2)
    query_width = QUERY_HEADS * HEAD_SIZE
    keys_width = KEY_VALUE_HEADS * HEAD_SIZE
    query_table = 2.5 * jax.random.truncated_normal(key_query, -3.0, 3.0, (SEQUENCE_LENGTH, query_width), jnp.float32)
    key_rows_table = jax.random.truncated_normal(key_keys, -3.0, 3.0, (SEQUENCE_LENGTH, keys_width), jnp.float32)
    return (query_table, key_rows_table)


def draw_queries(key, part):
    return make_pair(key)[0].astype(jnp.bfloat16)


def draw_keys(key, part):
    return make_pair(key)[1].astype(jnp.bfloat16)


def with_ends(values, rng, smallest, top_value):
    longest = values.shape.index(max(values.shape))
    spots = []
    for shift in (0, 1):
        where = [jax.random.randint(jax.random.fold_in(rng, axis), (), 0, length) for axis, length in enumerate(values.shape)]
        where[longest] = (where[longest] + shift) % values.shape[longest]
        spots.append(tuple(where))
    return values.at[spots[0]].set(smallest).at[spots[1]].set(top_value)


def steps_of(own_key, extent, cuts, smallest, high):
    factor_of = 1.0
    for axis_at, blocks in cuts:
        draws = jax.random.uniform(jax.random.fold_in(jax.random.fold_in(own_key, 6), axis_at), (blocks,), jnp.float32, smallest / len(cuts), high / len(cuts))
        factor_of = factor_of * jnp.repeat(jnp.exp(draws), extent[axis_at] // blocks).reshape((-1,) + (1,) * (len(extent) - 1 - axis_at))
    return factor_of


def noise(stream_key, dims, spread, bound, pieces=(), kind=jnp.bfloat16):
    values = jax.random.normal(stream_key, dims, jnp.float32) * spread
    if len(pieces) > 0:
        values = steps_of(stream_key, dims, pieces, -0.22, 0.18) * values
    return jnp.clip(values, min=-bound, max=bound).astype(kind)


def setup_inputs(seed: int = 0, part: int = 0) -> dict:
    splits = jax.random.split(jax.random.key(seed), 7)
    own_keys = jax.random.split(jax.random.fold_in(splits[6], part), 7)
    queries = draw_queries(jax.random.fold_in(jax.random.fold_in(splits[6], part), 71), part)
    keys = draw_keys(jax.random.fold_in(jax.random.fold_in(splits[6], part), 71), part)
    values = noise(own_keys[2], (SEQUENCE_LENGTH, KEY_VALUE_HEADS * HEAD_SIZE), 1.0, 4.0, ((0, 64),))
    out_packed = with_ends(jax.random.randint(splits[3], (QUERY_HEADS * HEAD_SIZE, DO // 8), -2147483648, 2147483647), jax.random.fold_in(splits[3], 1), -2147483648, 2147483646).astype(jnp.int32)
    out_scales = jnp.clip(jnp.exp(jax.random.uniform(splits[4], (QUERY_HEADS * HEAD_SIZE // GROUP, DO), jnp.float32, math.log(0.0029907227), math.log(0.029907227))), 0.0029907227, 0.029907227).astype(jnp.bfloat16)
    hadamard_signs = with_ends(jax.random.randint(splits[5], (QUERY_HEADS * HEAD_SIZE,), 0, 2), jax.random.fold_in(splits[5], 1), 0, 1).astype(jnp.int32)
    return {"queries": queries, "keys": keys, "values": values, "out_packed": out_packed, "out_scales": out_scales, "hadamard_signs": hadamard_signs}


def sylvester(block_count):
    index = jnp.arange(block_count, dtype=jnp.int32)
    both = jnp.bitwise_and(index[:, None], index[None, :])
    parity = jnp.zeros((block_count, block_count), jnp.int32)
    for bit_number in range(block_count.bit_length() - 1):
        parity = jnp.bitwise_xor(parity, jnp.bitwise_and(jnp.right_shift(both, bit_number), 1))
    return (1 - 2 * parity).astype(jnp.float32)

def rotate(attention, hadamard_signs):
    block_count = attention.shape[0]
    signed = attention.astype(jnp.float32) * (2 * hadamard_signs - 1).astype(jnp.float32)
    inner = jnp.einsum('rhd,de->rhe', signed.reshape(block_count, QUERY_HEADS, HEAD_SIZE), sylvester(HEAD_SIZE), precision=lax.Precision.HIGHEST)
    outer = jnp.einsum('gh,rhe->rge', sylvester(QUERY_HEADS), inner, precision=lax.Precision.HIGHEST)
    return (outer * (1.0 / math.sqrt(QUERY_HEADS * HEAD_SIZE))).reshape(block_count, QUERY_HEADS * HEAD_SIZE).astype(jnp.bfloat16)

def dequantize(packed, scale_rows):
    fields = [jnp.bitwise_and(jnp.right_shift(packed, 4 * nibble), 15) for nibble in range(8)]
    levels = jnp.concatenate(fields, axis=1) - 8
    return (levels.astype(jnp.float32) * scale_rows.astype(jnp.float32)).astype(jnp.bfloat16)

def reference(queries, keys, values, out_packed, out_scales, hadamard_signs):
    head_group = QUERY_HEADS // KEY_VALUE_HEADS
    block_number = math.gcd(SEQUENCE_LENGTH, 128)
    scale = 1.0 / math.sqrt(HEAD_SIZE)
    gathered_keys = keys.astype(jnp.float32).reshape(SEQUENCE_LENGTH, KEY_VALUE_HEADS, HEAD_SIZE)
    gathered_values = values.astype(jnp.float32).reshape(SEQUENCE_LENGTH, KEY_VALUE_HEADS, HEAD_SIZE)
    key_positions = jnp.arange(SEQUENCE_LENGTH, dtype=jnp.int32)

    def attend(start_offset):
        query_tile = lax.dynamic_slice_in_dim(queries, start_offset, block_number, 0).astype(jnp.float32).reshape(block_number, KEY_VALUE_HEADS, head_group, HEAD_SIZE)
        scores = jnp.einsum('qkgd,nkd->kgqn', query_tile, gathered_keys, precision=lax.Precision.HIGHEST) * scale
        query_positions = start_offset + jnp.arange(block_number, dtype=jnp.int32)
        allowed = query_positions[:, None] >= key_positions[None, :]
        scores = jnp.where(allowed, scores, -jnp.inf)
        largest = lax.optimization_barrier(jnp.max(scores, axis=-1, keepdims=True))
        weights = jnp.exp(scores - largest)
        totals = lax.optimization_barrier(jnp.sum(weights, axis=-1))
        rounded = lax.optimization_barrier(weights.astype(jnp.bfloat16)).astype(jnp.float32)
        summed = jnp.einsum('kgqn,nkd->qkgd', rounded, gathered_values, precision=lax.Precision.HIGHEST)
        summed = summed / jnp.transpose(totals, (2, 0, 1))[..., None]
        return summed.reshape(block_number, QUERY_HEADS * HEAD_SIZE).astype(jnp.bfloat16)
    starts = jnp.arange(SEQUENCE_LENGTH // block_number, dtype=jnp.int32) * block_number
    attention = lax.map(attend, starts).reshape(SEQUENCE_LENGTH, QUERY_HEADS * HEAD_SIZE)
    rotated = rotate(attention, hadamard_signs)
    scale_rows = jnp.repeat(out_scales, GROUP, axis=0)
    weight = dequantize(out_packed, scale_rows)
    return jnp.dot(rotated, weight, preferred_element_type=jnp.float32).astype(jnp.bfloat16)
```

```python
import math

import jax
import jax.numpy as jnp
from jax import lax
from jax.experimental import pallas as pl
from jax.experimental.pallas import tpu as pltpu
from jax.sharding import Mesh, PartitionSpec as P

HEAD = 128
KV_HEADS = 4
CORES = 2
LOCAL_KV = KV_HEADS // CORES
TILES = 8
WIDE = 8
DEEP = 4
SWAP = [(0, 1), (1, 0)]
MASKED = -1e30


def sylvester(n):
    index = jnp.arange(n, dtype=jnp.int32)
    both = jnp.bitwise_and(index[:, None], index[None, :])
    parity = jnp.zeros((n, n), jnp.int32)
    for bit in range(n.bit_length() - 1):
        parity = jnp.bitwise_xor(parity, jnp.bitwise_and(jnp.right_shift(both, bit), 1))
    return 1 - 2 * parity


def halves(c, mine, got):
    first = jnp.where(c == 0, mine, got)
    second = jnp.where(c == 0, got, mine)
    return first, second


def swap_half(x, c, width):
    mine = lax.dynamic_slice_in_dim(x, c * width, width, 1)
    other = lax.dynamic_slice_in_dim(x, (1 - c) * width, width, 1)
    got = lax.ppermute(other, "core", SWAP)
    return mine, got


def attend_pass(q_ref, block, m_ref, l_ref, acc_ref, h, base, rows, first):
    half = block.shape[0] // 2
    keys = jnp.concatenate([block[:half, :half], block[:half, half:]], axis=0)
    key2 = jnp.concatenate([keys, keys], axis=1)
    value_t = block[half:, :]
    spots = [pl.ds(base + t * rows, rows) for t in range(TILES)]
    scores = [
        jnp.dot(key2, q_ref[h, :, at], preferred_element_type=jnp.float32) for at in spots
    ]
    news, fadings, totals, rounded = [], [], [], []
    for at, s in zip(spots, scores):
        if first:
            key_pos = lax.broadcasted_iota(jnp.int32, s.shape, 0)
            row_pos = lax.broadcasted_iota(jnp.int32, s.shape, 1)
            s = jnp.where(key_pos <= row_pos, s, MASKED)
        new = jnp.max(s, axis=0, keepdims=True)
        if not first:
            old = m_ref[h, :, at]
            new = jnp.maximum(old, new)
            fadings.append(jnp.exp2(old - new))
        weights = jnp.exp2(s - new)
        news.append(new)
        totals.append(jnp.sum(weights, axis=0, keepdims=True))
        rounded.append(weights.astype(jnp.bfloat16))
    sums = [jnp.dot(value_t, w, preferred_element_type=jnp.float32) for w in rounded]
    if not first:
        totals = [l_ref[h, :, at] * f + t for at, f, t in zip(spots, fadings, totals)]
        sums = [acc_ref[h, :, at] * f + v for at, f, v in zip(spots, fadings, sums)]
    for at, new, total, summed in zip(spots, news, totals, sums):
        m_ref[h, :, at] = new
        l_ref[h, :, at] = total
        acc_ref[h, :, at] = summed


def first_kernel(tiles, rows, q_ref, own_ref, m_ref, l_ref, acc_ref):
    parts = tiles // TILES

    def body(i, carry):
        h = i // parts
        base = pl.multiple_of((i % parts) * (TILES * rows), TILES * rows)
        attend_pass(q_ref, own_ref[h], m_ref, l_ref, acc_ref, h, base, rows, True)
        return carry

    lax.fori_loop(0, LOCAL_KV * parts, body, 0)


def step_kernel(tiles, rows, chips, step, n_blocks, z_ref, q_ref, *refs):
    block_refs = refs[:n_blocks]
    m_in, l_in, acc_in, m_ref, l_ref, acc_ref = refs[n_blocks:]
    parts = tiles // TILES
    per_block = LOCAL_KV * parts
    m_ref[...] = m_in[...]
    l_ref[...] = l_in[...]
    acc_ref[...] = acc_in[...]
    z = z_ref[0]
    low = jnp.where(z >= step, 0, 1)
    high = jnp.where(z + step >= chips, 2, 1) if n_blocks == 2 else 1

    def body(i, carry):
        b = i // per_block
        h = (i // parts) % LOCAL_KV
        base = pl.multiple_of((i % parts) * (TILES * rows), TILES * rows)
        block = block_refs[0][h]
        if n_blocks == 2:
            block = jnp.where(b == 0, block, block_refs[1][h])
        attend_pass(q_ref, block, m_ref, l_ref, acc_ref, h, base, rows, False)
        return carry

    lax.fori_loop(low * per_block, high * per_block, body, 0)


VMEM = pl.BlockSpec(memory_space=pltpu.VMEM)
SMEM = pl.BlockSpec(memory_space=pltpu.SMEM)


def state_shapes(lanes):
    return (
        jax.ShapeDtypeStruct((LOCAL_KV, 1, lanes), jnp.float32),
        jax.ShapeDtypeStruct((LOCAL_KV, 1, lanes), jnp.float32),
        jax.ShapeDtypeStruct((LOCAL_KV, HEAD, lanes), jnp.float32),
    )


def cost(lanes, rows, n_blocks):
    return pl.CostEstimate(
        flops=LOCAL_KV * lanes * rows * n_blocks * HEAD * 4,
        bytes_accessed=LOCAL_KV * lanes * HEAD * 12,
        transcendentals=LOCAL_KV * lanes * rows * n_blocks,
    )


def attend_first(q, own, rows):
    lanes = q.shape[2]
    tiles = lanes // rows
    return pl.pallas_call(
        lambda *r: first_kernel(tiles, rows, *r),
        out_shape=state_shapes(lanes),
        in_specs=[VMEM] * 2,
        out_specs=(VMEM,) * 3,
        compiler_params=pltpu.CompilerParams(vmem_limit_bytes=24 << 20),
        cost_estimate=cost(lanes, rows, 1),
        name="attend_first",
    )(q, own)


def attend_step(z, q, blocks, state, rows, chips, step):
    lanes = q.shape[2]
    tiles = lanes // rows
    n = len(blocks)
    return pl.pallas_call(
        lambda *r: step_kernel(tiles, rows, chips, step, n, *r),
        out_shape=state_shapes(lanes),
        in_specs=[SMEM] + [VMEM] * (1 + n + 3),
        out_specs=(VMEM,) * 3,
        input_output_aliases={2 + n + i: i for i in range(3)},
        compiler_params=pltpu.CompilerParams(vmem_limit_bytes=24 << 20),
        cost_estimate=cost(lanes, rows, n),
        name="attend_step",
    )(z, q, *blocks, *state)


def block_kernel(core_ref, mine_ref, got_ref, out_ref):
    c = core_ref[0]
    first = jnp.where(c == 0, mine_ref[...], got_ref[...])
    second = jnp.where(c == 0, got_ref[...], mine_ref[...])
    n = first.shape[0]
    for h in range(LOCAL_KV):
        at = h * HEAD
        out_ref[h, :n, :] = jnp.concatenate([first[:, at : at + HEAD], second[:, at : at + HEAD]], 1)
        at += LOCAL_KV * HEAD
        turned = [
            jnp.transpose(x[:, at : at + HEAD].astype(jnp.float32)).astype(jnp.bfloat16)
            for x in (first, second)
        ]
        out_ref[h, n:, :] = jnp.concatenate(turned, 1)


def make_blocks(c, mine, got):
    n = mine.shape[0]
    return pl.pallas_call(
        block_kernel,
        out_shape=jax.ShapeDtypeStruct((LOCAL_KV, n + HEAD, 2 * n), jnp.bfloat16),
        in_specs=[SMEM] + [VMEM] * 2,
        out_specs=VMEM,
        compiler_params=pltpu.CompilerParams(vmem_limit_bytes=8 << 20),
        name="blocks",
    )(c, mine, got)


def query_kernel(heads, core_ref, mine_ref, got_ref, out_ref):
    c = core_ref[0]
    n = mine_ref.shape[0]
    scale = math.log2(math.e) / math.sqrt(HEAD)
    for j in range(heads):
        h, at = j // (heads // LOCAL_KV), (j % (heads // LOCAL_KV)) * CORES * n
        columns = slice(j * HEAD, (j + 1) * HEAD)
        mine, got = mine_ref[:, columns], got_ref[:, columns]
        both = [jnp.where(c == 0, mine, got), jnp.where(c == 0, got, mine)]
        turned = [jnp.transpose(x.astype(jnp.float32)) * scale for x in both]
        scaled = jnp.concatenate(turned, 1)
        upper = scaled.astype(jnp.bfloat16)
        lower = (scaled - upper.astype(jnp.float32)).astype(jnp.bfloat16)
        out_ref[h, :HEAD, at : at + CORES * n] = upper
        out_ref[h, HEAD:, at : at + CORES * n] = lower


def make_queries(c, mine, got):
    heads = mine.shape[1] // HEAD
    lanes = heads // LOCAL_KV * CORES * mine.shape[0]
    return pl.pallas_call(
        lambda *r: query_kernel(heads, *r),
        out_shape=jax.ShapeDtypeStruct((LOCAL_KV, 2 * HEAD, lanes), jnp.bfloat16),
        in_specs=[SMEM] + [VMEM] * 2,
        out_specs=VMEM,
        compiler_params=pltpu.CompilerParams(vmem_limit_bytes=16 << 20),
        name="queries",
    )(c, mine, got)


def finish_kernel(tiles, rows, l_ref, acc_ref, out_ref):
    for h in range(LOCAL_KV):
        for j in range(tiles):
            lanes = pl.ds(j * rows, rows)
            out_ref[h * tiles + j] = (acc_ref[h, :, lanes] / l_ref[h, :, lanes]).astype(jnp.bfloat16)


def finish(state, rows):
    _, totals, acc = state
    tiles = acc.shape[2] // rows
    return pl.pallas_call(
        lambda *r: finish_kernel(tiles, rows, *r),
        out_shape=jax.ShapeDtypeStruct((LOCAL_KV * tiles, HEAD, rows), jnp.bfloat16),
        in_specs=[VMEM] * 2,
        out_specs=VMEM,
        compiler_params=pltpu.CompilerParams(vmem_limit_bytes=24 << 20),
        name="finish",
    )(totals, acc)


def rotate_kernel(heads, rows, core_ref, mine_ref, got_ref, table_ref, out_ref, work_ref):
    c = core_ref[0]
    half = heads // CORES

    def inner(i, carry):
        for t in range(WIDE):
            h = i * WIDE + t
            mine = (h // half) == c
            source = jnp.where(mine, mine_ref[h % half], got_ref[h % half])
            work_ref[h] = jnp.dot(table_ref[h], source, preferred_element_type=jnp.float32)
        return carry

    lax.fori_loop(0, heads // WIDE, inner, 0)

    def mix(i, carry):
        at = pl.multiple_of((i // (rows // 128)) * 8, 8)
        lanes = pl.ds(pl.multiple_of((i % (rows // 128)) * 128, 128), 128)
        parts = [work_ref[h, pl.ds(at, 8), lanes] for h in range(heads)]
        span = 1
        while span < heads:
            parts = [
                parts[h] + parts[h + span] if not h & span else parts[h - span] - parts[h]
                for h in range(heads)
            ]
            span *= 2
        for h in range(heads):
            work_ref[h, pl.ds(at, 8), lanes] = parts[h]
        return carry

    lax.fori_loop(0, (HEAD // 8) * (rows // 128), mix, 0)
    scale = 1.0 / math.sqrt(heads * HEAD)

    def back(i, carry):
        turned = [jnp.transpose(work_ref[i * WIDE + t]) for t in range(WIDE)]
        for t in range(WIDE):
            out_ref[i * WIDE + t] = (turned[t] * scale).astype(jnp.bfloat16)
        return carry

    lax.fori_loop(0, heads // WIDE, back, 0)


def rotate(c, mine, got, table):
    heads, rows = table.shape[0], mine.shape[2]
    return pl.pallas_call(
        lambda *r: rotate_kernel(heads, rows, *r),
        out_shape=jax.ShapeDtypeStruct((heads, rows, HEAD), jnp.bfloat16),
        in_specs=[SMEM] + [VMEM] * 3,
        out_specs=VMEM,
        scratch_shapes=[pltpu.VMEM((heads, HEAD, rows), jnp.float32)],
        compiler_params=pltpu.CompilerParams(vmem_limit_bytes=24 << 20),
        name="rotate",
    )(c, mine, got, table)


def project_kernel(rotated_ref, scale_ref, packed_ref, out_ref, acc_ref):
    groups, _, width = packed_ref.shape
    fields = acc_ref.shape[0]
    acc_ref[...] = jnp.zeros_like(acc_ref)

    def body(i, carry):
        zs = [i * DEEP + t for t in range(DEEP)]
        left = jnp.concatenate([rotated_ref[z] for z in zs], axis=1)
        words = [packed_ref[z] ^ jnp.int32(-2004318072) for z in zs]
        for k in range(fields):
            parts = []
            for z, word in zip(zs, words):
                level = jnp.right_shift(jnp.left_shift(word, 28 - 4 * k), 28)
                scale = scale_ref[z, pl.ds(k, 1), :]
                parts.append((level.astype(jnp.float32) * scale).astype(jnp.bfloat16))
            weight = jnp.concatenate(parts, axis=0)
            acc_ref[k] += jnp.dot(left, weight, preferred_element_type=jnp.float32)
        return carry

    lax.fori_loop(0, groups // DEEP, body, 0)
    for k in range(fields):
        out_ref[:, k * width : (k + 1) * width] = acc_ref[k].astype(jnp.bfloat16)


def project(rotated, scales, packed):
    rows, fields, width = rotated.shape[1], scales.shape[1], packed.shape[2]
    return pl.pallas_call(
        project_kernel,
        out_shape=jax.ShapeDtypeStruct((rows, fields * width), jnp.bfloat16),
        in_specs=[VMEM] * 3,
        out_specs=VMEM,
        scratch_shapes=[pltpu.VMEM((fields, rows, width), jnp.float32)],
        compiler_params=pltpu.CompilerParams(vmem_limit_bytes=32 << 20),
        name="project",
    )(rotated, scales, packed)


def local_of(chips):
    up_ring = [(i, (i + 1) % chips) for i in range(chips)]
    down_ring = [(i, (i - 1) % chips) for i in range(chips)]

    def local(queries, keys, values, out_packed, out_scales, hadamard_signs):
        c = lax.axis_index("core")
        core = c.reshape(1).astype(jnp.int32)
        z = lax.axis_index("z").reshape(1).astype(jnp.int32)
        own_rows = queries.shape[0]
        rows = CORES * own_rows
        heads = queries.shape[1] // HEAD
        local_heads = heads // CORES

        width = LOCAL_KV * HEAD
        own_kv = [lax.dynamic_slice_in_dim(x, c * width, width, 1) for x in (keys, values)]
        other_kv = [lax.dynamic_slice_in_dim(x, (1 - c) * width, width, 1) for x in (keys, values)]
        kv_got = lax.ppermute(jnp.concatenate(other_kv, 1), "core", SWAP)
        own = make_blocks(core, jnp.concatenate(own_kv, 1), kv_got)

        packed_width = out_packed.shape[1] // CORES
        packed_mine, packed_got = swap_half(out_packed, c, packed_width)
        packed_own = jnp.concatenate(halves(c, packed_mine, packed_got), 0)
        packed_all = lax.all_gather(packed_own, "z", axis=0, tiled=False)

        q = make_queries(core, *swap_half(queries, c, local_heads * HEAD))

        signs = (2 * hadamard_signs - 1).reshape(heads, 1, HEAD)
        table = (sylvester(HEAD)[None] * signs).astype(jnp.bfloat16)
        scales = out_scales.reshape(out_scales.shape[0], 8, CORES, packed_width)
        scales = lax.dynamic_index_in_dim(scales, c, 2, keepdims=False).astype(jnp.float32)

        state = attend_first(q, own, rows)
        largest = [state[0]]
        up = down = own
        for step in range(1, chips // 2 + 1):
            if step >= 2:
                up, down, _ = lax.optimization_barrier((up, down, largest[step - 2]))
            up = lax.ppermute(up, "z", up_ring)
            arrived = [up]
            if step < chips - step:
                down = lax.ppermute(down, "z", down_ring)
                arrived.append(down)
            state = attend_step(z, q, arrived, state, rows, chips, step)
            largest.append(state[0])

        mine = finish(state, rows)
        got = lax.ppermute(mine, "core", SWAP)
        rotated = rotate(core, mine, got, table)
        mixed = project(rotated, scales, packed_all)

        keep = lax.dynamic_slice_in_dim(mixed, c * own_rows, own_rows, 0)
        give = lax.dynamic_slice_in_dim(mixed, (1 - c) * own_rows, own_rows, 0)
        taken = lax.ppermute(give, "core", SWAP)
        low, high = halves(c, keep, taken)
        low = low.reshape(own_rows, 8, 1, packed_width)
        high = high.reshape(own_rows, 8, 1, packed_width)
        return jnp.concatenate([low, high], 2).reshape(own_rows, 8 * CORES * packed_width)

    return local


def solution(mesh):
    groups, chips = mesh.shape["groups"], mesh.shape["blk"] // CORES
    inner = Mesh(mesh.devices.reshape(groups, chips, CORES), ("groups", "z", "core"))
    rows = P(("groups", "z", "core"), None)
    return jax.shard_map(
        local_of(chips),
        mesh=inner,
        in_specs=(rows, rows, rows, P(("z", "core"), None), P(), P()),
        out_specs=rows,
        check_vma=False,
    )
```

```python
import math

import jax
import jax.numpy as jnp
from jax import lax
from jax.experimental import pallas as pl
from jax.experimental.pallas import tpu as pltpu
from jax.sharding import Mesh, PartitionSpec as P

HEAD = 128
KV_HEADS = 4
CORES = 2
LOCAL_KV = KV_HEADS // CORES
TILES = 8
WIDE = 8
DEEP = 4
SWAP = [(0, 1), (1, 0)]
MASKED = -1e30


def sylvester(n):
    index = jnp.arange(n, dtype=jnp.int32)
    both = jnp.bitwise_and(index[:, None], index[None, :])
    parity = jnp.zeros((n, n), jnp.int32)
    for bit in range(n.bit_length() - 1):
        parity = jnp.bitwise_xor(parity, jnp.bitwise_and(jnp.right_shift(both, bit), 1))
    return 1 - 2 * parity


def halves(c, mine, got):
    first = jnp.where(c == 0, mine, got)
    second = jnp.where(c == 0, got, mine)
    return first, second


def swap_half(x, c, width):
    mine = lax.dynamic_slice_in_dim(x, c * width, width, 1)
    other = lax.dynamic_slice_in_dim(x, (1 - c) * width, width, 1)
    got = lax.ppermute(other, "core", SWAP)
    return mine, got


def attend_pass(q_ref, block, m_ref, l_ref, acc_ref, h, base, rows, first):
    half = block.shape[0] // 2
    keys = jnp.concatenate([block[:half, :half], block[:half, half:]], axis=0)
    key2 = jnp.concatenate([keys, keys], axis=1)
    value_t = block[half:, :]
    spots = [pl.ds(base + t * rows, rows) for t in range(TILES)]
    scores = [
        jnp.dot(key2, q_ref[h, :, at], preferred_element_type=jnp.float32) for at in spots
    ]
    news, fadings, totals, rounded = [], [], [], []
    for at, s in zip(spots, scores):
        if first:
            key_pos = lax.broadcasted_iota(jnp.int32, s.shape, 0)
            row_pos = lax.broadcasted_iota(jnp.int32, s.shape, 1)
            s = jnp.where(key_pos <= row_pos, s, MASKED)
        new = jnp.max(s, axis=0, keepdims=True)
        if not first:
            old = m_ref[h, :, at]
            new = jnp.maximum(old, new)
            fadings.append(jnp.exp2(old - new))
        weights = jnp.exp2(s - new)
        news.append(new)
        totals.append(jnp.sum(weights, axis=0, keepdims=True))
        rounded.append(weights.astype(jnp.bfloat16))
    sums = [jnp.dot(value_t, w, preferred_element_type=jnp.float32) for w in rounded]
    if not first:
        totals = [l_ref[h, :, at] * f + t for at, f, t in zip(spots, fadings, totals)]
        sums = [acc_ref[h, :, at] * f + v for at, f, v in zip(spots, fadings, sums)]
    for at, new, total, summed in zip(spots, news, totals, sums):
        m_ref[h, :, at] = new
        l_ref[h, :, at] = total
        acc_ref[h, :, at] = summed


def first_kernel(tiles, rows, q_ref, own_ref, m_ref, l_ref, acc_ref):
    parts = tiles // TILES

    def body(i, carry):
        h = i // parts
        base = pl.multiple_of((i % parts) * (TILES * rows), TILES * rows)
        attend_pass(q_ref, own_ref[h], m_ref, l_ref, acc_ref, h, base, rows, True)
        return carry

    lax.fori_loop(0, LOCAL_KV * parts, body, 0)


def step_kernel(tiles, rows, chips, step, n_blocks, z_ref, q_ref, *refs):
    block_refs = refs[:n_blocks]
    m_in, l_in, acc_in, m_ref, l_ref, acc_ref = refs[n_blocks:]
    parts = tiles // TILES
    per_block = LOCAL_KV * parts
    m_ref[...] = m_in[...]
    l_ref[...] = l_in[...]
    acc_ref[...] = acc_in[...]
    z = z_ref[0]
    low = jnp.where(z >= step, 0, 1)
    high = jnp.where(z + step >= chips, 2, 1) if n_blocks == 2 else 1

    def body(i, carry):
        b = i // per_block
        h = (i // parts) % LOCAL_KV
        base = pl.multiple_of((i % parts) * (TILES * rows), TILES * rows)
        block = block_refs[0][h]
        if n_blocks == 2:
            block = jnp.where(b == 0, block, block_refs[1][h])
        attend_pass(q_ref, block, m_ref, l_ref, acc_ref, h, base, rows, False)
        return carry

    lax.fori_loop(low * per_block, high * per_block, body, 0)


VMEM = pl.BlockSpec(memory_space=pltpu.VMEM)
SMEM = pl.BlockSpec(memory_space=pltpu.SMEM)


def state_shapes(lanes):
    return (
        jax.ShapeDtypeStruct((LOCAL_KV, 1, lanes), jnp.float32),
        jax.ShapeDtypeStruct((LOCAL_KV, 1, lanes), jnp.float32),
        jax.ShapeDtypeStruct((LOCAL_KV, HEAD, lanes), jnp.float32),
    )


def cost(lanes, rows, n_blocks):
    return pl.CostEstimate(
        flops=LOCAL_KV * lanes * rows * n_blocks * HEAD * 4,
        bytes_accessed=LOCAL_KV * lanes * HEAD * 12,
        transcendentals=LOCAL_KV * lanes * rows * n_blocks,
    )


def attend_first(q, own, rows):
    lanes = q.shape[2]
    tiles = lanes // rows
    return pl.pallas_call(
        lambda *r: first_kernel(tiles, rows, *r),
        out_shape=state_shapes(lanes),
        in_specs=[VMEM] * 2,
        out_specs=(VMEM,) * 3,
        compiler_params=pltpu.CompilerParams(vmem_limit_bytes=24 << 20),
        cost_estimate=cost(lanes, rows, 1),
        name="attend_first",
    )(q, own)


def attend_step(z, q, blocks, state, rows, chips, step):
    lanes = q.shape[2]
    tiles = lanes // rows
    n = len(blocks)
    return pl.pallas_call(
        lambda *r: step_kernel(tiles, rows, chips, step, n, *r),
        out_shape=state_shapes(lanes),
        in_specs=[SMEM] + [VMEM] * (1 + n + 3),
        out_specs=(VMEM,) * 3,
        input_output_aliases={2 + n + i: i for i in range(3)},
        compiler_params=pltpu.CompilerParams(vmem_limit_bytes=24 << 20),
        cost_estimate=cost(lanes, rows, n),
        name="attend_step",
    )(z, q, *blocks, *state)


def block_kernel(core_ref, mine_ref, got_ref, out_ref):
    c = core_ref[0]
    first = jnp.where(c == 0, mine_ref[...], got_ref[...])
    second = jnp.where(c == 0, got_ref[...], mine_ref[...])
    n = first.shape[0]
    for h in range(LOCAL_KV):
        at = h * HEAD
        out_ref[h, :n, :] = jnp.concatenate([first[:, at : at + HEAD], second[:, at : at + HEAD]], 1)
        at += LOCAL_KV * HEAD
        turned = [
            jnp.transpose(x[:, at : at + HEAD].astype(jnp.float32)).astype(jnp.bfloat16)
            for x in (first, second)
        ]
        out_ref[h, n:, :] = jnp.concatenate(turned, 1)


def make_blocks(c, mine, got):
    n = mine.shape[0]
    return pl.pallas_call(
        block_kernel,
        out_shape=jax.ShapeDtypeStruct((LOCAL_KV, n + HEAD, 2 * n), jnp.bfloat16),
        in_specs=[SMEM] + [VMEM] * 2,
        out_specs=VMEM,
        compiler_params=pltpu.CompilerParams(vmem_limit_bytes=8 << 20),
        name="blocks",
    )(c, mine, got)


def query_kernel(heads, core_ref, mine_ref, got_ref, out_ref):
    c = core_ref[0]
    n = mine_ref.shape[0]
    scale = math.log2(math.e) / math.sqrt(HEAD)
    for j in range(heads):
        h, at = j // (heads // LOCAL_KV), (j % (heads // LOCAL_KV)) * CORES * n
        columns = slice(j * HEAD, (j + 1) * HEAD)
        mine, got = mine_ref[:, columns], got_ref[:, columns]
        both = [jnp.where(c == 0, mine, got), jnp.where(c == 0, got, mine)]
        turned = [jnp.transpose(x.astype(jnp.float32)) * scale for x in both]
        scaled = jnp.concatenate(turned, 1)
        upper = scaled.astype(jnp.bfloat16)
        lower = (scaled - upper.astype(jnp.float32)).astype(jnp.bfloat16)
        out_ref[h, :HEAD, at : at + CORES * n] = upper
        out_ref[h, HEAD:, at : at + CORES * n] = lower


def make_queries(c, mine, got):
    heads = mine.shape[1] // HEAD
    lanes = heads // LOCAL_KV * CORES * mine.shape[0]
    return pl.pallas_call(
        lambda *r: query_kernel(heads, *r),
        out_shape=jax.ShapeDtypeStruct((LOCAL_KV, 2 * HEAD, lanes), jnp.bfloat16),
        in_specs=[SMEM] + [VMEM] * 2,
        out_specs=VMEM,
        compiler_params=pltpu.CompilerParams(vmem_limit_bytes=16 << 20),
        name="queries",
    )(c, mine, got)


def last_kernel(tiles, rows, chips, step, n_blocks, z_ref, q_ref, *refs):
    out_ref, m_ref, l_ref, acc_ref = refs[n_blocks + 3 :]
    state_refs = refs[: n_blocks + 3] + (m_ref, l_ref, acc_ref)
    step_kernel(tiles, rows, chips, step, n_blocks, z_ref, q_ref, *state_refs)
    for h in range(LOCAL_KV):
        for j in range(tiles):
            lanes = pl.ds(j * rows, rows)
            out_ref[h * tiles + j] = (acc_ref[h, :, lanes] / l_ref[h, :, lanes]).astype(jnp.bfloat16)


def attend_last(z, q, blocks, state, rows, chips, step):
    lanes = q.shape[2]
    tiles = lanes // rows
    n = len(blocks)
    return pl.pallas_call(
        lambda *r: last_kernel(tiles, rows, chips, step, n, *r),
        out_shape=jax.ShapeDtypeStruct((LOCAL_KV * tiles, HEAD, rows), jnp.bfloat16),
        in_specs=[SMEM] + [VMEM] * (1 + n + 3),
        out_specs=VMEM,
        scratch_shapes=[pltpu.VMEM(x.shape, x.dtype) for x in state_shapes(lanes)],
        compiler_params=pltpu.CompilerParams(vmem_limit_bytes=24 << 20),
        cost_estimate=cost(lanes, rows, n),
        name="attend_last",
    )(z, q, *blocks, *state)


def rotate_kernel(heads, rows, core_ref, mine_ref, got_ref, table_ref, out_ref, work_ref):
    c = core_ref[0]
    half = heads // CORES

    def inner(i, carry):
        for t in range(WIDE):
            h = i * WIDE + t
            mine = (h // half) == c
            source = jnp.where(mine, mine_ref[h % half], got_ref[h % half])
            work_ref[h] = jnp.dot(table_ref[h], source, preferred_element_type=jnp.float32)
        return carry

    lax.fori_loop(0, heads // WIDE, inner, 0)

    def mix(i, carry):
        at = pl.multiple_of((i // (rows // 128)) * 8, 8)
        lanes = pl.ds(pl.multiple_of((i % (rows // 128)) * 128, 128), 128)
        parts = [work_ref[h, pl.ds(at, 8), lanes] for h in range(heads)]
        span = 1
        while span < heads:
            parts = [
                parts[h] + parts[h + span] if not h & span else parts[h - span] - parts[h]
                for h in range(heads)
            ]
            span *= 2
        for h in range(heads):
            work_ref[h, pl.ds(at, 8), lanes] = parts[h]
        return carry

    lax.fori_loop(0, (HEAD // 8) * (rows // 128), mix, 0)
    scale = 1.0 / math.sqrt(heads * HEAD)

    def back(i, carry):
        turned = [jnp.transpose(work_ref[i * WIDE + t]) for t in range(WIDE)]
        for t in range(WIDE):
            out_ref[i * WIDE + t] = (turned[t] * scale).astype(jnp.bfloat16)
        return carry

    lax.fori_loop(0, heads // WIDE, back, 0)


def rotate(c, mine, got, table):
    heads, rows = table.shape[0], mine.shape[2]
    return pl.pallas_call(
        lambda *r: rotate_kernel(heads, rows, *r),
        out_shape=jax.ShapeDtypeStruct((heads, rows, HEAD), jnp.bfloat16),
        in_specs=[SMEM] + [VMEM] * 3,
        out_specs=VMEM,
        scratch_shapes=[pltpu.VMEM((heads, HEAD, rows), jnp.float32)],
        compiler_params=pltpu.CompilerParams(vmem_limit_bytes=24 << 20),
        name="rotate",
    )(c, mine, got, table)


def project_kernel(rotated_ref, scale_ref, packed_ref, out_ref, acc_ref):
    groups, _, width = packed_ref.shape
    fields = acc_ref.shape[0]
    acc_ref[...] = jnp.zeros_like(acc_ref)

    def body(i, carry):
        zs = [i * DEEP + t for t in range(DEEP)]
        left = jnp.concatenate([rotated_ref[z] for z in zs], axis=1)
        words = [packed_ref[z] ^ jnp.int32(-2004318072) for z in zs]
        for k in range(fields):
            parts = []
            for z, word in zip(zs, words):
                level = jnp.right_shift(jnp.left_shift(word, 28 - 4 * k), 28)
                scale = scale_ref[z, pl.ds(k, 1), :]
                parts.append((level.astype(jnp.float32) * scale).astype(jnp.bfloat16))
            weight = jnp.concatenate(parts, axis=0)
            acc_ref[k] += jnp.dot(left, weight, preferred_element_type=jnp.float32)
        return carry

    lax.fori_loop(0, groups // DEEP, body, 0)
    for k in range(fields):
        out_ref[:, k * width : (k + 1) * width] = acc_ref[k].astype(jnp.bfloat16)


def project(rotated, scales, packed):
    rows, fields, width = rotated.shape[1], scales.shape[1], packed.shape[2]
    return pl.pallas_call(
        project_kernel,
        out_shape=jax.ShapeDtypeStruct((rows, fields * width), jnp.bfloat16),
        in_specs=[VMEM] * 3,
        out_specs=VMEM,
        scratch_shapes=[pltpu.VMEM((fields, rows, width), jnp.float32)],
        compiler_params=pltpu.CompilerParams(vmem_limit_bytes=32 << 20),
        name="project",
    )(rotated, scales, packed)


def weave_kernel(width, core_ref, keep_ref, taken_ref, out_ref):
    c = core_ref[0]
    for k in range(keep_ref.shape[1] // width):
        columns = slice(k * width, (k + 1) * width)
        keep, taken = keep_ref[:, columns], taken_ref[:, columns]
        at = 2 * k * width
        out_ref[:, at : at + width] = jnp.where(c == 0, keep, taken)
        out_ref[:, at + width : at + 2 * width] = jnp.where(c == 0, taken, keep)


def weave(c, keep, taken, width):
    n, columns = keep.shape
    return pl.pallas_call(
        lambda *r: weave_kernel(width, *r),
        out_shape=jax.ShapeDtypeStruct((n, CORES * columns), keep.dtype),
        in_specs=[SMEM] + [VMEM] * 2,
        out_specs=VMEM,
        compiler_params=pltpu.CompilerParams(vmem_limit_bytes=8 << 20),
        name="weave",
    )(c, keep, taken)


def local_of(chips):
    up_ring = [(i, (i + 1) % chips) for i in range(chips)]
    down_ring = [(i, (i - 1) % chips) for i in range(chips)]

    def local(queries, keys, values, out_packed, out_scales, hadamard_signs):
        c = lax.axis_index("core")
        core = c.reshape(1).astype(jnp.int32)
        z = lax.axis_index("z").reshape(1).astype(jnp.int32)
        own_rows = queries.shape[0]
        rows = CORES * own_rows
        heads = queries.shape[1] // HEAD
        local_heads = heads // CORES

        width = LOCAL_KV * HEAD
        own_kv = [lax.dynamic_slice_in_dim(x, c * width, width, 1) for x in (keys, values)]
        other_kv = [lax.dynamic_slice_in_dim(x, (1 - c) * width, width, 1) for x in (keys, values)]
        kv_got = lax.ppermute(jnp.concatenate(other_kv, 1), "core", SWAP)
        own = make_blocks(core, jnp.concatenate(own_kv, 1), kv_got)

        packed_width = out_packed.shape[1] // CORES
        packed_mine, packed_got = swap_half(out_packed, c, packed_width)
        packed_own = jnp.concatenate(halves(c, packed_mine, packed_got), 0)
        packed_all = lax.all_gather(packed_own, "z", axis=0, tiled=False)

        q = make_queries(core, *swap_half(queries, c, local_heads * HEAD))

        signs = (2 * hadamard_signs - 1).reshape(heads, 1, HEAD)
        table = (sylvester(HEAD)[None] * signs).astype(jnp.bfloat16)
        scales = out_scales.reshape(out_scales.shape[0], 8, CORES, packed_width)
        scales = lax.dynamic_index_in_dim(scales, c, 2, keepdims=False).astype(jnp.float32)

        state = attend_first(q, own, rows)
        largest = [state[0]]
        up = down = own
        for step in range(1, chips // 2 + 1):
            if step >= 2:
                up, _ = lax.optimization_barrier((up, largest[step - 2]))
            up = lax.ppermute(up, "z", up_ring)
            arrived = [up]
            if step < chips - step:
                if step >= 2:
                    down, _ = lax.optimization_barrier((down, largest[step - 2]))
                down = lax.ppermute(down, "z", down_ring)
                arrived.append(down)
            if step < chips // 2:
                state = attend_step(z, q, arrived, state, rows, chips, step)
                largest.append(state[0])
            else:
                mine = attend_last(z, q, arrived, state, rows, chips, step)

        got = lax.ppermute(mine, "core", SWAP)
        rotated = rotate(core, mine, got, table)
        mixed = project(rotated, scales, packed_all)

        keep = lax.dynamic_slice_in_dim(mixed, c * own_rows, own_rows, 0)
        give = lax.dynamic_slice_in_dim(mixed, (1 - c) * own_rows, own_rows, 0)
        taken = lax.ppermute(give, "core", SWAP)
        return weave(core, keep, taken, packed_width)

    return local


def solution(mesh):
    groups, chips = mesh.shape["groups"], mesh.shape["blk"] // CORES
    inner = Mesh(mesh.devices.reshape(groups, chips, CORES), ("groups", "z", "core"))
    rows = P(("groups", "z", "core"), None)
    return jax.shard_map(
        local_of(chips),
        mesh=inner,
        in_specs=(rows, rows, rows, P(("z", "core"), None), P(), P()),
        out_specs=rows,
        check_vma=False,
    )
```
